256 devices in a mesh: docs: 64 (over x, z, core), rep: 4 (over y).
Axes of the slice: x: 4, y: 4, z: 8, core: 2. Of those that a mesh axis runs over, the one named last changes fastest.
Arguments:
- embeddings: bfloat16 [262144, 4096], P(('docs', 'rep')), may hold values from -6 to 6
- pca_basis: bfloat16 [4096, 256], replicated, may hold values from -0.09375 to 0.09375
- cluster: int32 [262144, 1], P(('docs', 'rep')), may hold values from 0 to 255; in each aligned block of 1024 rows (0 to 1023, 1024 to 2047, ...) at most 8 rows name the same one
- doc_index: int32 [262144], P(('docs', 'rep')), may hold values from 0 to 262143, each once
Outputs:
- nearest_sim: float32 [262144], P(('docs', 'rep'))
The draws below stay inside these ranges and needn't reach their ends.
Inputs may be any that keep to these rules, and one draw needn't show every extreme that they name: In each device's block of 1024 rows no cluster is named by more than 8 rows, a bound that some block reaches. `doc_index`: each document number appears once.
All inputs are finite; a program needn't handle non-finite values.
Results may differ from the reference program's by a relative error of at most 0.0014.
Values may be sent and summed in bfloat16 or wider, within the bound.
A program may use at most 64 MiB of HBM per device.

```python
import math
import jax
import jax.numpy as jnp
import numpy as np
from jax import lax

E = 4096
P_SIZE = 256
DOC_DEV = 1024
CLUSTERS = 256
MOST = 8
DOCS = 262144
CAP = 2048


def levels(own_key, extent, cuts, least, largest):
    loudness, own = 1.0, jax.random.fold_in(own_key, 6)
    for position, blocks in cuts:
        heights = jnp.exp(jax.random.uniform(jax.random.fold_in(own, position), (blocks,), jnp.float32, least / len(cuts), largest / len(cuts)))
        loudness = loudness * jnp.repeat(heights, extent[position] // blocks).reshape([-1 if axis == position else 1 for axis in range(len(extent))])
    return loudness


def routed_block(own_key, own, number, rows, number_of, top, most, lean):
    sequence = jax.random.permutation(own_key, number_of)
    crowded, ordinary = shares(number_of, rows * top, most, lean, True), shares(number_of, rows * top, most, lean, False)
    places = jnp.arange(number_of)

    def named(sizes, turn):
        used = int((sizes > 0).sum())
        fixed = max(1, used // 4)
        passed = fixed + (places - fixed + turn * (used - fixed)) % max(1, number_of - fixed)
        return jnp.zeros((number_of,), jnp.int32).at[sequence[jnp.where(places < fixed, places, passed)]].set(jnp.asarray(sizes, jnp.int32))

    sizes = jnp.where(number % 4 == 0, named(crowded, number // 4), named(ordinary, number - number // 4 - 1))
    mixed = jax.random.permutation(jax.random.fold_in(own, 3), number_of)
    donor, sink = mixed[0:number_of // 2 * 2:2], mixed[1:number_of // 2 * 2:2]
    room = jnp.minimum(sizes[donor] - 1, most - sizes[sink]) // 2
    room = jnp.where((donor == sequence[0]) | (sink == sequence[0]) | (sizes[sink] == 0), 0, jnp.maximum(room, 0))
    passed = jax.random.randint(jax.random.fold_in(own, 4), (number_of // 2,), 0, 1 << 20) % (room + 1)
    sizes = sizes.at[donor].add(-passed).at[sink].add(passed)
    labels = jnp.searchsorted(jnp.cumsum(sizes), jnp.arange(rows * top), side="right").astype(jnp.int32)
    table = labels.reshape(top, rows).T
    table = table[jax.random.permutation(jax.random.fold_in(own, 1), rows)]
    turn = jax.random.randint(jax.random.fold_in(own, 2), (rows, 1), 0, top)
    return jnp.take_along_axis(table, (jnp.arange(top)[None, :] + turn) % top, axis=1)


def shares(count, total, most, slope, full):
    weights = [(1 << 20) // math.isqrt(standing ** slope) + 1 for standing in range(1, count + 1)]
    largest = most if full else min(most, max(-(-total // count), total * weights[0] // sum(weights)))
    least = 1 if total - largest >= count - 1 else 0
    given, spare = [largest] + [least] * (count - 1), total - largest - least * (count - 1)
    while spare > 0:
        free = [i for i in range(1, count) if given[i] < largest] or [i for i in range(1, count) if given[i] < most]
        pool, left = sum([weights[i] for i in free]), spare
        for i in free:
            extra = min(most - given[i], max(1, left * weights[i] // pool), spare)
            given[i] = given[i] + extra
            spare = spare - extra
    return np.array(given)


def scatter_about(stream_key, extent, width, bound, shards=(), held_as=jnp.bfloat16):
    array = jax.random.normal(stream_key, extent, jnp.float32) * width
    if len(shards) > 0:
        array = levels(stream_key, extent, shards, -0.22, 0.18) * array
    return jnp.clip(array, min=-bound, max=bound).astype(held_as)


def setup_inputs(seed: int = 0) -> dict:
    seeds = jax.random.split(jax.random.key(seed), 5)
    embeddings = scatter_about(seeds[0], (DOCS, E), 1.0, 6.0, ((0, 256),))
    pca_basis = scatter_about(seeds[1], (E, P_SIZE), E ** -0.5, 0.09375)
    cluster_keys = jax.random.split(jax.random.fold_in(seeds[2], 1), DOCS // DOC_DEV)
    cluster_turns = jax.random.permutation(jax.random.fold_in(seeds[2], 3), DOCS // DOC_DEV)
    cluster = jax.vmap(lambda own, number: routed_block(jax.random.fold_in(seeds[2], 2), own, number, DOC_DEV, CLUSTERS, 1, MOST, 2))(cluster_keys, cluster_turns).reshape((DOCS, 1))
    doc_index = jax.random.permutation(seeds[3], DOCS).astype(jnp.int32)
    return dict(embeddings=embeddings, pca_basis=pca_basis, cluster=cluster, doc_index=doc_index)


def project_rows(embeddings, pca_basis):
    blocks = embeddings.reshape(-1, DOC_DEV, embeddings.shape[1])
    basis_wide = pca_basis.astype(jnp.float32)

    def single(block):
        return jnp.dot(block.astype(jnp.float32), basis_wide, precision=lax.Precision.HIGHEST)
    projected = lax.map(single, blocks).reshape(-1, pca_basis.shape[1])
    scaled = projected * lax.rsqrt(lax.optimization_barrier(jnp.sum(projected * projected, axis=1, keepdims=True)) + 1e-06)
    return scaled.astype(jnp.bfloat16)

def reference(embeddings, pca_basis, cluster, doc_index):
    unit_rows = project_rows(embeddings, pca_basis)
    cluster_id = cluster[:, 0].astype(jnp.int32)
    order = jnp.argsort(cluster_id * DOCS + doc_index).astype(jnp.int32)
    sorted_rows = unit_rows[order]
    sorted_ids = cluster_id[order]
    counts = jnp.zeros((CLUSTERS,), jnp.int32).at[cluster_id].add(1)
    starts = (jnp.cumsum(counts) - counts).astype(jnp.int32)
    padded = jnp.concatenate([sorted_rows, jnp.zeros((CAP, sorted_rows.shape[1]), sorted_rows.dtype)], axis=0)
    places = jnp.arange(CAP, dtype=jnp.int32)

    def per_cluster(inputs):
        begin, amount = inputs
        members = lax.dynamic_slice_in_dim(padded, begin, CAP, 0)
        scores = jnp.dot(members, members.T, preferred_element_type=jnp.float32)
        allowed = (places[None, :] < places[:, None]) & (places[None, :] < amount)
        return lax.optimization_barrier(jnp.max(jnp.where(allowed, scores, -1.0), axis=1))
    results = lax.map(per_cluster, (starts, counts))
    offsets = jnp.arange(DOCS, dtype=jnp.int32) - starts[sorted_ids]
    values = results[sorted_ids, offsets]
    return jnp.zeros_like(values).at[order].set(values)
```

```python
import jax
import jax.numpy as jnp
from jax import lax
from jax.experimental import pallas as pl
from jax.experimental.pallas import tpu as pltpu
from jax.sharding import PartitionSpec as P

MESH = pl.DeviceIdType.MESH
NX, NY, NZ, NC = 4, 4, 8, 2
NP = NX * NY * NC
DEPTH = 8
ROWS = 1024
PC = 256
E = 4096
BLK = NP * DEPTH
NEMB = 4
EROWS = ROWS // NEMB
ORDER = (4, 3, 5, 2, 6, 1, 7, 0)
BIG = float(2**30)
f32, bf16, i32 = jnp.float32, jnp.bfloat16, jnp.int32


def dot(a, b, ca, cb):
    return lax.dot_general(a, b, (((ca,), (cb,)), ((), ())), preferred_element_type=f32)


def wait_bytes(ref, sem):
    pltpu.make_async_copy(ref, ref, sem).wait()


def kernel(
    cl_ref, ix_ref, emb_ref, bas_ref, out_ref,
    ebuf, bbuf, unit, place, upper, slot_ref, hplane,
    idx_p, idx_in, idx_z, idx_rec, col,
    send, recv1, recv2, rows, best, bestcol,
    ret_row, ret_z, ret_p, ret_c,
    e_sem, b_sem, ip_s, ip_r, iz_s, iz_r, rp_s, rp_r, rz_s, rz_r, bz_s, bz_r, bp_s, bp_r,
):
    d = lax.axis_index("docs")
    y = lax.axis_index("rep")
    core = lax.rem(d, NC)
    z = lax.rem(d // NC, NZ)
    x = d // (NC * NZ)
    p = (x * NY + y) * NC + core

    def at_z(z2):
        return ((x * NZ + z2) * NC + core, y)

    def at_p(p2):
        return (((p2 // (NY * NC)) * NZ + z) * NC + lax.rem(p2, NC), lax.rem(p2 // NC, NY))

    def turn_z(step):
        return lax.rem(z + step, NZ)

    def turn_p(step):
        return lax.rem(p + step, NP)

    barrier = pltpu.get_barrier_semaphore()
    for step in range(1, NZ):
        pl.semaphore_signal(barrier, inc=1, device_id=at_z(turn_z(step)), device_id_type=MESH)

    @pl.loop(1, NP)
    def _(step):
        pl.semaphore_signal(barrier, inc=1, device_id=at_p(turn_p(step)), device_id_type=MESH)

    basis_copy = pltpu.make_async_copy(bas_ref, bbuf, b_sem)
    basis_copy.start()
    emb_copies = [
        pltpu.make_async_copy(emb_ref.at[pl.ds(n * EROWS, EROWS)], ebuf.at[n], e_sem.at[n])
        for n in range(NEMB)
    ]
    for copy in emb_copies:
        copy.start()

    cl = cl_ref[...]
    one_hot = (lax.broadcasted_iota(i32, (NZ * NP, ROWS), 0) == cl).astype(f32)
    upper[...] = (
        lax.broadcasted_iota(i32, (ROWS, ROWS), 0) < lax.broadcasted_iota(i32, (ROWS, ROWS), 1)
    ).astype(f32).astype(bf16)
    earlier = dot(one_hot.astype(bf16), upper[...], 1, 0)
    rank = jnp.sum(earlier * one_hot, axis=0, keepdims=True).astype(i32)
    slot = cl * DEPTH + rank
    slot_ref[...] = slot
    plane = slot // BLK
    inside = lax.rem(slot, BLK)
    place[...] = (lax.broadcasted_iota(i32, (BLK, ROWS), 0) == inside).astype(f32).astype(bf16)
    number = ix_ref[...] + 1
    mine = lax.broadcasted_iota(i32, (128, ROWS), 0) == plane
    total = jnp.zeros((BLK, 128), f32)
    for part, weight in ((number // 4096, 4096.0), (lax.rem(number // 64, 64), 64.0), (lax.rem(number, 64), 1.0)):
        held = jnp.where(mine, part.astype(f32), 0.0).astype(bf16)
        total = total + weight * dot(place[...], held, 1, 1)
    idx_p[...] = total.reshape(NP, DEPTH, 128)

    pl.semaphore_wait(barrier, NZ - 1 + NP - 1)

    @pl.loop(1, NP)
    def _(step):
        p2 = turn_p(step)
        pltpu.make_async_remote_copy(
            src_ref=idx_p.at[p2], dst_ref=idx_in.at[p], send_sem=ip_s, recv_sem=ip_r,
            device_id=at_p(p2), device_id_type=MESH,
        ).start()

    idx_in[p] = idx_p[p]

    basis_copy.wait()

    @pl.loop(0, NEMB)
    def _(n):
        pltpu.make_async_copy(emb_ref.at[pl.ds(n * EROWS, EROWS)], ebuf.at[n], e_sem.at[n]).wait()
        projected = jnp.dot(ebuf[n], bbuf[...], preferred_element_type=f32)
        scale = lax.rsqrt(jnp.sum(projected * projected, axis=1, keepdims=True) + 1e-06)
        unit[pl.ds(pl.multiple_of(n * EROWS, EROWS), EROWS), :] = (projected * scale).astype(bf16)

    for step in ORDER:
        z2 = turn_z(step)
        picks = (lax.broadcasted_iota(i32, (BLK, ROWS), 0) + z2 * BLK == slot_ref[...]).astype(f32)
        chosen = jnp.dot(picks.astype(bf16), unit[...], preferred_element_type=f32)
        send[z2] = chosen.reshape(NP, DEPTH, PC).astype(bf16)

        @pl.loop(1, NP)
        def _(turn, z2=z2):
            p2 = turn_p(turn)
            pltpu.make_async_remote_copy(
                src_ref=send.at[z2, p2], dst_ref=recv1.at[z2, p], send_sem=rp_s, recv_sem=rp_r.at[z2],
                device_id=at_p(p2), device_id_type=MESH,
            ).start()

        recv1[z2, p] = send[z2, p]
        if step == ORDER[0]:
            wait_bytes(idx_in.at[pl.ds(0, NP - 1)], ip_r)
            turned = idx_in[...].reshape(BLK, 128).T
            for k in range(NZ):
                idx_z[k] = turned[k : k + 1, :]
            for k, far in enumerate(ORDER):
                if far:
                    pltpu.make_async_remote_copy(
                        src_ref=idx_z.at[turn_z(far)], dst_ref=idx_rec.at[k], send_sem=iz_s, recv_sem=iz_r,
                        device_id=at_z(turn_z(far)), device_id_type=MESH,
                    ).start()
                else:
                    idx_rec[k] = idx_z[z]

    for k, step in enumerate(ORDER):
        z2 = turn_z(step)
        wait_bytes(recv1.at[z2, pl.ds(0, NP - 1)], rp_r.at[z2])
        if step:
            pltpu.make_async_remote_copy(
                src_ref=recv1.at[z2], dst_ref=recv2.at[k], send_sem=rz_s.at[k], recv_sem=rz_r.at[k],
                device_id=at_z(z2), device_id_type=MESH,
            ).start()

    wait_bytes(idx_rec.at[pl.ds(0, NZ - 1)], iz_r)

    @pl.loop(0, NZ)
    def _(k):
        row = idx_rec[k]
        row = jnp.where(row == 0.0, BIG, row)
        idx_rec[k] = row
        col[k] = jnp.broadcast_to(row, (128, BLK)).T
        best[k] = jnp.full((8, BLK), -1.0, f32)
        bestcol[k] = jnp.full((BLK, 128), -1.0, f32)

    def pair(b, a, same):
        scores = dot(rows[b], rows[a], 1, 1)
        cb = col[b]
        ra = idx_rec[a]
        over_rows = []
        over_cols = None
        for h in range(BLK // 128):
            lanes = slice(h * 128, (h + 1) * 128)
            s = scores[:, lanes]
            allowed = cb < ra[:, lanes]
            over_rows.append(jnp.max(jnp.where(allowed, s, -1.0).reshape(BLK // 8, 8, 128), axis=0))
            if not same:
                other = jnp.where(allowed, -1.0, s)
                over_cols = other if over_cols is None else jnp.maximum(over_cols, other)
        best[a] = jnp.maximum(best[a], jnp.concatenate(over_rows, axis=1))
        if not same:
            bestcol[b] = jnp.maximum(bestcol[b], over_cols)

    def arrived(k):
        pair(k, k, True)

        @pl.loop(0, k)
        def _(b):
            pair(b, k, False)

    rows[NZ - 1] = recv1[z].reshape(BLK, PC)
    pair(NZ - 1, NZ - 1, True)

    @pl.loop(0, NZ - 1)
    def _(k):
        wait_bytes(recv2.at[k], rz_r.at[k])
        rows[k] = recv2[k].reshape(BLK, PC)
        arrived(k)
        pair(NZ - 1, k, False)

    for k, step in enumerate(ORDER):
        final = jnp.maximum(
            jnp.max(best[k], axis=0, keepdims=True), jnp.max(bestcol[k].T, axis=0, keepdims=True)
        )
        ret_row[k] = final
        z2 = lax.rem(z + NZ - step, NZ)
        if step:
            pltpu.make_async_remote_copy(
                src_ref=ret_row.at[k], dst_ref=ret_z.at[z], send_sem=bz_s, recv_sem=bz_r,
                device_id=at_z(z2), device_id_type=MESH,
            ).start()
        else:
            ret_z[z] = final
    wait_bytes(ret_z.at[pl.ds(0, NZ - 1)], bz_r)
    ret_p[...] = jnp.concatenate(
        [ret_z[...].reshape(NZ, BLK), jnp.zeros((128 - NZ, BLK), f32)], axis=0
    ).T.reshape(NP, DEPTH, 128)

    @pl.loop(1, NP)
    def _(step):
        p2 = turn_p(step)
        pltpu.make_async_remote_copy(
            src_ref=ret_p.at[p2], dst_ref=ret_c.at[p], send_sem=bp_s, recv_sem=bp_r,
            device_id=at_p(p2), device_id_type=MESH,
        ).start()

    ret_c[p] = ret_p[p]
    wait_bytes(ret_c.at[pl.ds(0, NP - 1)], bp_r)
    whole = ret_c[...].reshape(BLK, 128).T[:NZ, :]
    high = whole.astype(bf16)
    rest = whole - high.astype(f32)
    mid = rest.astype(bf16)
    low = (rest - mid.astype(f32)).astype(bf16)
    got = jnp.zeros((NZ, ROWS), f32)
    for piece in (high, mid, low):
        got = got + jnp.dot(piece, place[...], preferred_element_type=f32)
    slots = slot_ref[...]
    mask = lax.broadcasted_iota(i32, (NZ, ROWS), 0) == slots // BLK
    out_ref[...] = jnp.sum(jnp.where(mask, got, 0.0), axis=0, keepdims=True)

    wait_bytes(idx_p.at[pl.ds(0, NP - 1)], ip_s)
    wait_bytes(idx_z.at[pl.ds(0, NZ - 1)], iz_s)
    wait_bytes(send.at[:, pl.ds(0, NP - 1)], rp_s)
    for k, step in enumerate(ORDER):
        if step:
            wait_bytes(recv1.at[k], rz_s.at[k])
    wait_bytes(ret_row.at[pl.ds(0, NZ - 1)], bz_s)
    wait_bytes(ret_p.at[pl.ds(0, NP - 1)], bp_s)


def on_device(embeddings, pca_basis, cluster, doc_index):
    vmem = pl.BlockSpec(memory_space=pltpu.VMEM)
    hbm = pl.BlockSpec(memory_space=pl.ANY)
    dma = pltpu.SemaphoreType.DMA
    out = pl.pallas_call(
        kernel,
        out_shape=jax.ShapeDtypeStruct((1, ROWS), f32),
        in_specs=[vmem, vmem, hbm, hbm],
        out_specs=vmem,
        scratch_shapes=[
            pltpu.VMEM((NEMB, EROWS, E), bf16),
            pltpu.VMEM((E, PC), bf16),
            pltpu.VMEM((ROWS, PC), bf16),
            pltpu.VMEM((BLK, ROWS), bf16),
            pltpu.VMEM((ROWS, ROWS), bf16),
            pltpu.VMEM((1, ROWS), i32),
            pltpu.VMEM((128, ROWS), bf16),
            pltpu.VMEM((NP, DEPTH, 128), f32),
            pltpu.VMEM((NP, DEPTH, 128), f32),
            pltpu.VMEM((NZ, 1, BLK), f32),
            pltpu.VMEM((NZ, 1, BLK), f32),
            pltpu.VMEM((NZ, BLK, 128), f32),
            pltpu.VMEM((NZ, NP, DEPTH, PC), bf16),
            pltpu.VMEM((NZ, NP, DEPTH, PC), bf16),
            pltpu.VMEM((NZ, NP, DEPTH, PC), bf16),
            pltpu.VMEM((NZ, BLK, PC), bf16),
            pltpu.VMEM((NZ, 8, BLK), f32),
            pltpu.VMEM((NZ, BLK, 128), f32),
            pltpu.VMEM((NZ, 1, BLK), f32),
            pltpu.VMEM((NZ, 1, BLK), f32),
            pltpu.VMEM((NP, DEPTH, 128), f32),
            pltpu.VMEM((NP, DEPTH, 128), f32),
            dma((NEMB,)), dma, dma, dma, dma, dma, dma, dma((NZ,)), dma((NZ,)), dma((NZ,)),
            dma, dma, dma, dma,
        ],
        compiler_params=pltpu.CompilerParams(
            collective_id=0, has_side_effects=True, vmem_limit_bytes=60 * 2**20
        ),
    )(cluster.reshape(1, ROWS), doc_index.reshape(1, ROWS), embeddings, pca_basis)
    return out.reshape(ROWS)


def solution(mesh):
    return jax.shard_map(
        on_device,
        mesh=mesh,
        in_specs=(P(("docs", "rep"), None), P(), P(("docs", "rep"), None), P(("docs", "rep"))),
        out_specs=P(("docs", "rep")),
        check_vma=False,
    )
```

```python
import jax
import jax.numpy as jnp
from jax import lax
from jax.experimental import pallas as pl
from jax.experimental.pallas import tpu as pltpu
from jax.sharding import PartitionSpec as P

MESH = pl.DeviceIdType.MESH
NX, NY, NZ, NC = 4, 4, 8, 2
NP = NX * NY * NC
DEPTH = 8
ROWS = 1024
PC = 256
E = 4096
BLK = NP * DEPTH
NEMB = 8
DEEP = E // NEMB
EROWS = 256
FAR = (4,)
NEAR = (3, 5, 2, 6, 1, 7)
ORDER = (0, 3, 5, 4, 2, 6, 1, 7)
BIG = float(2**30)
f32, bf16, i32 = jnp.float32, jnp.bfloat16, jnp.int32


def dot(a, b, ca, cb):
    return lax.dot_general(a, b, (((ca,), (cb,)), ((), ())), preferred_element_type=f32)


def wait_bytes(ref, sem):
    pltpu.make_async_copy(ref, ref, sem).wait()


def kernel(
    cl_ref, ix_ref, emb_ref, bas_ref, out_ref,
    ebuf, bbuf, proj, unit, which, upper, slot_ref,
    idx_p, idx_in, idx_z, idx_rec, col,
    send, recv1, zin, fin, rows, best, bestcol,
    ret_row, ret_z, ret_p, ret_c,
    e_sem, b_sem, ip_s, ip_r, iz_s, iz_r, rp_s, rp_r, zi_s, zi_r, fw_s, fin_r, rz_s,
    bz_s, bz_r, bp_s, bp_r,
):
    d = lax.axis_index("docs")
    y = lax.axis_index("rep")
    core = lax.rem(d, NC)
    z = lax.rem(d // NC, NZ)
    x = d // (NC * NZ)
    p = (x * NY + y) * NC + core

    def at_z(z2):
        return ((x * NZ + z2) * NC + core, y)

    def at_p(p2):
        return (((p2 // (NY * NC)) * NZ + z) * NC + lax.rem(p2, NC), lax.rem(p2 // NC, NY))

    def turn_z(step):
        return lax.rem(z + step, NZ)

    def turn_p(step):
        return lax.rem(p + step, NP)

    def to_z(src, dst, send_sem, recv_sem, z2):
        pltpu.make_async_remote_copy(
            src_ref=src, dst_ref=dst, send_sem=send_sem, recv_sem=recv_sem,
            device_id=at_z(z2), device_id_type=MESH,
        ).start()

    def to_plane(src, dst, send_sem, recv_sem):
        @pl.loop(1, NP)
        def _(step):
            p2 = turn_p(step)
            pltpu.make_async_remote_copy(
                src_ref=src.at[p2], dst_ref=dst.at[p], send_sem=send_sem, recv_sem=recv_sem,
                device_id=at_p(p2), device_id_type=MESH,
            ).start()

        dst[p] = src[p]

    def all_but_one(ref):
        return ref.at[pl.ds(0, NP - 1)]


    def depth_in(n):
        part = pl.ds(n * DEEP, DEEP)
        return (
            pltpu.make_async_copy(bas_ref.at[part], bbuf.at[part], b_sem.at[n]),
            pltpu.make_async_copy(emb_ref.at[:, part], ebuf.at[:, part], e_sem.at[n]),
        )

    for n in range(NEMB):
        for copy in depth_in(n):
            copy.start()
    barrier = pltpu.get_barrier_semaphore()
    for step in range(1, NZ):
        pl.semaphore_signal(barrier, inc=1, device_id=at_z(turn_z(step)), device_id_type=MESH)

    @pl.loop(1, NP)
    def _(step):
        pl.semaphore_signal(barrier, inc=1, device_id=at_p(turn_p(step)), device_id_type=MESH)

    cl = cl_ref[...]
    one_hot = (lax.broadcasted_iota(i32, (NZ * NP, ROWS), 0) == cl).astype(f32)
    upper[...] = (
        lax.broadcasted_iota(i32, (ROWS, ROWS), 0) < lax.broadcasted_iota(i32, (ROWS, ROWS), 1)
    ).astype(f32).astype(bf16)
    earlier = dot(one_hot.astype(bf16), upper[...], 1, 0)
    rank = jnp.sum(earlier * one_hot, axis=0, keepdims=True).astype(i32)
    slot_ref[...] = cl * DEPTH + rank
    lane = rank * NZ + cl // NP
    which[...] = (lax.broadcasted_iota(i32, (NP, ROWS), 0) == lax.rem(cl, NP)).astype(f32).astype(bf16)
    number = ix_ref[...] + 1
    mine = lax.broadcasted_iota(i32, (128, ROWS), 0) == lane
    total = jnp.zeros((NP, 128), f32)
    for part, weight in ((number // 4096, 4096.0), (lax.rem(number // 64, 64), 64.0), (lax.rem(number, 64), 1.0)):
        held = jnp.where(mine, part.astype(f32), 0.0).astype(bf16)
        total = total + weight * dot(which[...], held, 1, 1)
    idx_p[...] = total.reshape(NP, 1, 128)

    for n in range(NEMB):
        for copy in depth_in(n):
            copy.wait()
        part = slice(n * DEEP, (n + 1) * DEEP)
        partial = jnp.dot(ebuf[:, part], bbuf[part, :], preferred_element_type=f32)
        proj[...] = proj[...] + partial if n else partial
    for n in range(ROWS // EROWS):
        part = slice(n * EROWS, (n + 1) * EROWS)
        projected = proj[part, :]
        scale = lax.rsqrt(jnp.sum(projected * projected, axis=1, keepdims=True) + 1e-06)
        unit[part, :] = (projected * scale).astype(bf16)

    def put(step):
        z2 = turn_z(step)
        picks = (lax.broadcasted_iota(i32, (BLK, ROWS), 0) == slot_ref[...] - z2 * BLK).astype(f32)
        chosen = jnp.dot(picks.astype(bf16), unit[...], preferred_element_type=f32)
        send[z2] = chosen.reshape(NP, DEPTH, PC).astype(bf16)

    pl.semaphore_wait(barrier, NZ - 1 + NP - 1)

    def own_lanes():
        return lax.broadcasted_iota(i32, (BLK, 128), 1) // NZ == lax.rem(
            lax.broadcasted_iota(i32, (BLK, 128), 0), DEPTH
        )

    def pass_numbers():
        wait_bytes(all_but_one(idx_in), ip_r)
        wide = jnp.broadcast_to(idx_in[...], (NP, DEPTH, 128)).reshape(BLK, 128)
        keep = own_lanes()
        turned = jnp.where(keep, wide, 0.0).T.reshape(128 // NZ, NZ, BLK).sum(axis=0)
        for k in range(NZ):
            idx_z[k] = turned[k : k + 1, :]
        for k, step in enumerate(ORDER):
            if step:
                to_z(idx_z.at[turn_z(step)], idx_rec.at[k], iz_s, iz_r, turn_z(step))
            else:
                idx_rec[k] = idx_z[z]

    def onward(step):
        k = ORDER.index(step)
        z2 = turn_z(step)
        wait_bytes(all_but_one(recv1.at[z2]), rp_r.at[z2])
        to_z(recv1.at[z2], fin.at[k], rz_s.at[k], fin_r.at[k], z2)

    def across(step):
        j, k = FAR.index(step), ORDER.index(step)
        wait_bytes(zin.at[j], zi_r.at[j])
        to_plane(zin.at[j], fin.at[k], fw_s, fin_r.at[k])

    def spread_put(step):
        put(step)
        z2 = turn_z(step)
        to_plane(send.at[z2], recv1.at[z2], rp_s, rp_r.at[z2])

    put(FAR[0])
    to_z(send.at[turn_z(FAR[0])], zin.at[0], zi_s.at[0], zi_r.at[0], turn_z(FAR[0]))
    spread_put(3)
    to_plane(idx_p, idx_in, ip_s, ip_r)
    spread_put(5)
    spread_put(2)
    spread_put(6)
    pass_numbers()
    onward(3)
    spread_put(1)
    onward(5)
    spread_put(7)
    onward(2)
    spread_put(0)
    across(4)
    onward(6)
    onward(1)
    onward(7)

    wait_bytes(idx_rec.at[pl.ds(0, NZ - 1)], iz_r)

    @pl.loop(0, NZ)
    def _(k):
        row = idx_rec[k]
        row = jnp.where(row == 0.0, BIG, row)
        idx_rec[k] = row
        col[k] = jnp.broadcast_to(row, (128, BLK)).T
        best[k] = jnp.full((8, BLK), -1.0, f32)
        bestcol[k] = jnp.full((BLK, 128), -1.0, f32)

    def pair(b, a, same):
        scores = dot(rows[b], rows[a], 1, 1)
        cb = col[b]
        ra = idx_rec[a]
        over_rows = []
        over_cols = None
        for h in range(BLK // 128):
            lanes = slice(h * 128, (h + 1) * 128)
            s = scores[:, lanes]
            allowed = cb < ra[:, lanes]
            over_rows.append(jnp.max(jnp.where(allowed, s, -1.0).reshape(BLK // 8, 8, 128), axis=0))
            if not same:
                other = jnp.where(allowed, -1.0, s)
                over_cols = other if over_cols is None else jnp.maximum(over_cols, other)
        best[a] = jnp.maximum(best[a], jnp.concatenate(over_rows, axis=1))
        if not same:
            bestcol[b] = jnp.maximum(bestcol[b], over_cols)

    def meet(k):
        pair(k, k, True)
        for b in range(k):
            pair(b, k, False)

    for k, step in enumerate(ORDER):
        if step == 0:
            wait_bytes(all_but_one(recv1.at[z]), rp_r.at[z])
            rows[k] = recv1[z].reshape(BLK, PC)
        else:
            if step in FAR:
                wait_bytes(all_but_one(fin.at[k]), fin_r.at[k])
            else:
                wait_bytes(fin.at[k], fin_r.at[k])
            rows[k] = fin[k].reshape(BLK, PC)
        meet(k)

    finals = [
        jnp.maximum(
            jnp.max(best[k], axis=0, keepdims=True), jnp.max(bestcol[k].T, axis=0, keepdims=True)
        )
        for k in range(NZ)
    ]
    for k in range(1, NZ):
        ret_row[k] = finals[k]
    for k in range(1, NZ):
        to_z(ret_row.at[k], ret_z.at[z], bz_s, bz_r, turn_z(NZ - ORDER[k]))
    ret_z[z] = finals[0]
    wait_bytes(ret_z.at[pl.ds(0, NZ - 1)], bz_r)
    stacked = ret_z[...].reshape(NZ, BLK)
    spread = jnp.concatenate([stacked] * (128 // NZ), axis=0).T
    ret_p[...] = jnp.where(own_lanes(), spread, 0.0).reshape(NP, DEPTH, 128).sum(axis=1, keepdims=True)
    to_plane(ret_p, ret_c, bp_s, bp_r)
    wait_bytes(all_but_one(ret_c), bp_r)
    whole = ret_c[...].reshape(NP, 128).T[: NZ * DEPTH, :]
    high = whole.astype(bf16)
    rest = whole - high.astype(f32)
    mid = rest.astype(bf16)
    low = (rest - mid.astype(f32)).astype(bf16)
    got = jnp.zeros((NZ * DEPTH, ROWS), f32)
    for piece in (high, mid, low):
        got = got + jnp.dot(piece, which[...], preferred_element_type=f32)
    slots = slot_ref[...]
    lanes = lax.rem(slots, DEPTH) * NZ + slots // BLK
    mask = lax.broadcasted_iota(i32, (NZ * DEPTH, ROWS), 0) == lanes
    out_ref[...] = jnp.sum(jnp.where(mask, got, 0.0), axis=0, keepdims=True)

    wait_bytes(all_but_one(idx_p), ip_s)
    wait_bytes(idx_z.at[pl.ds(0, NZ - 1)], iz_s)
    wait_bytes(send.at[pl.ds(0, len(NEAR) + 1), pl.ds(0, NP - 1)], rp_s)
    for j in range(len(FAR)):
        wait_bytes(zin.at[j], zi_s.at[j])
    wait_bytes(zin.at[:, pl.ds(0, NP - 1)], fw_s)
    for step in NEAR:
        k = ORDER.index(step)
        wait_bytes(fin.at[k], rz_s.at[k])
    wait_bytes(ret_row.at[pl.ds(0, NZ - 1)], bz_s)
    wait_bytes(all_but_one(ret_p), bp_s)


def on_device(embeddings, pca_basis, cluster, doc_index):
    vmem = pl.BlockSpec(memory_space=pltpu.VMEM)
    hbm = pl.BlockSpec(memory_space=pl.ANY)
    dma = pltpu.SemaphoreType.DMA
    out = pl.pallas_call(
        kernel,
        out_shape=jax.ShapeDtypeStruct((1, ROWS), f32),
        in_specs=[vmem, vmem, hbm, hbm],
        out_specs=vmem,
        scratch_shapes=[
            pltpu.VMEM((ROWS, E), bf16),
            pltpu.VMEM((E, PC), bf16),
            pltpu.VMEM((ROWS, PC), f32),
            pltpu.VMEM((ROWS, PC), bf16),
            pltpu.VMEM((NP, ROWS), bf16),
            pltpu.VMEM((ROWS, ROWS), bf16),
            pltpu.VMEM((1, ROWS), i32),
            pltpu.VMEM((NP, 1, 128), f32),
            pltpu.VMEM((NP, 1, 128), f32),
            pltpu.VMEM((NZ, 1, BLK), f32),
            pltpu.VMEM((NZ, 1, BLK), f32),
            pltpu.VMEM((NZ, BLK, 128), f32),
            pltpu.VMEM((NZ, NP, DEPTH, PC), bf16),
            pltpu.VMEM((NZ, NP, DEPTH, PC), bf16),
            pltpu.VMEM((len(FAR), NP, DEPTH, PC), bf16),
            pltpu.VMEM((NZ, NP, DEPTH, PC), bf16),
            pltpu.VMEM((NZ, BLK, PC), bf16),
            pltpu.VMEM((NZ, 8, BLK), f32),
            pltpu.VMEM((NZ, BLK, 128), f32),
            pltpu.VMEM((NZ, 1, BLK), f32),
            pltpu.VMEM((NZ, 1, BLK), f32),
            pltpu.VMEM((NP, 1, 128), f32),
            pltpu.VMEM((NP, 1, 128), f32),
            dma((NEMB,)), dma((NEMB,)), dma, dma, dma, dma, dma, dma((NZ,)), dma((len(FAR),)), dma((len(FAR),)),
            dma, dma((NZ,)), dma((NZ,)), dma, dma, dma, dma,
        ],
        compiler_params=pltpu.CompilerParams(
            collective_id=0, has_side_effects=True, vmem_limit_bytes=60 * 2**20
        ),
    )(cluster.reshape(1, ROWS), doc_index.reshape(1, ROWS), embeddings, pca_basis)
    return out.reshape(ROWS)


def solution(mesh):
    return jax.shard_map(
        on_device,
        mesh=mesh,
        in_specs=(P(("docs", "rep"), None), P(), P(("docs", "rep"), None), P(("docs", "rep"))),
        out_specs=P(("docs", "rep")),
        check_vma=False,
    )
```

```python
import jax
import jax.numpy as jnp
from jax import lax
from jax.experimental import pallas as pl
from jax.experimental.pallas import tpu as pltpu
from jax.sharding import PartitionSpec as P

MESH = pl.DeviceIdType.MESH
NX, NY, NZ, NC = 4, 4, 8, 2
NP = NX * NY * NC
DEPTH = 8
ROWS = 1024
PC = 256
E = 4096
BLK = NP * DEPTH
NEMB = 8
EARLY = 0
DEEP = E // NEMB
EROWS = 256
ORDER = (0, 3, 5, 4, 2, 6, 1, 7)
FAR = 3
BIG = float(2**30)
f32, bf16, i32 = jnp.float32, jnp.bfloat16, jnp.int32


def dot(a, b, ca, cb):
    return lax.dot_general(a, b, (((ca,), (cb,)), ((), ())), preferred_element_type=f32)


def step_of(j):
    return NZ // 2 + (1 - 2 * (j % 2)) * ((j + 1) // 2)


def slot_of(j):
    return j + (j + 5) // 8


def wait_bytes(ref, sem):
    pltpu.make_async_copy(ref, ref, sem).wait()


def kernel(
    cl_hbm, ix_hbm, emb_ref, bas_ref, out_ref,
    cl_ref, ix_ref, ebuf, bbuf, proj, unit, which, upper, slot_ref,
    idx_p, idx_in, idx_z, idx_rec, col, colnow,
    send, recv1, zin, fin, rows, best, bestcol,
    ret_row, ret_z, ret_p, ret_c,
    n_sem, e_sem, b_sem, ip_s, ip_r, iz_s, iz_r, rp_s, rp_r, zi_s, zi_r, fw_s, fin_r, rz_s,
    bz_s, bz_r, bp_s, bp_r,
):
    d = lax.axis_index("docs")
    y = lax.axis_index("rep")
    core = lax.rem(d, NC)
    z = lax.rem(d // NC, NZ)
    x = d // (NC * NZ)
    p = (x * NY + y) * NC + core

    def at_z(z2):
        return ((x * NZ + z2) * NC + core, y)

    def turn_z(step):
        return lax.rem(z + step, NZ)

    beside = [
        (lax.rem(y + ky, NY), lax.rem(core + kc, NC)) for ky in range(NY) for kc in range(NC)
    ]
    beside = [(y2, y2 * NC + c2, z * NC + c2) for y2, c2 in beside]

    def each_beside(fn):
        def of_column(x2, some):
            for y2, place, deep in some:
                fn(x2 * (NY * NC) + place, (x2 * (NZ * NC) + deep, y2))

        of_column(x, beside[1:])

        @pl.loop(1, NX)
        def _(kx):
            of_column(lax.rem(x + kx, NX), beside)

    def to_z(src, dst, send_sem, recv_sem, z2):
        pltpu.make_async_remote_copy(
            src_ref=src, dst_ref=dst, send_sem=send_sem, recv_sem=recv_sem,
            device_id=at_z(z2), device_id_type=MESH,
        ).start()

    def to_plane(src, dst, send_sem, recv_sem):
        def to_one(p2, device):
            pltpu.make_async_remote_copy(
                src_ref=src.at[p2], dst_ref=dst.at[p], send_sem=send_sem, recv_sem=recv_sem,
                device_id=device, device_id_type=MESH,
            ).start()

        each_beside(to_one)
        dst[p] = src[p]

    def all_but_one(ref):
        return ref.at[pl.ds(0, NP - 1)]

    cl_copy = pltpu.make_async_copy(cl_hbm, cl_ref, n_sem.at[0])
    ix_copy = pltpu.make_async_copy(ix_hbm, ix_ref, n_sem.at[1])
    cl_copy.start()
    ix_copy.start()
    def depth_in(n):
        part = pl.ds(pl.multiple_of(n * DEEP, DEEP), DEEP)
        return (
            pltpu.make_async_copy(bas_ref.at[part], bbuf.at[part], b_sem.at[n]),
            pltpu.make_async_copy(emb_ref.at[:, part], ebuf.at[:, part], e_sem.at[n]),
        )

    for n in range(EARLY):
        for copy in depth_in(n):
            copy.start()
    barrier = pltpu.get_barrier_semaphore()
    for step in range(1, NZ):
        pl.semaphore_signal(barrier, inc=1, device_id=at_z(turn_z(step)), device_id_type=MESH)

    each_beside(
        lambda p2, device: pl.semaphore_signal(barrier, inc=1, device_id=device, device_id_type=MESH)
    )

    cl_copy.wait()
    ix_copy.wait()
    for n in range(EARLY, NEMB):
        for copy in depth_in(n):
            copy.start()
    cl = cl_ref[...]
    one_hot = (lax.broadcasted_iota(i32, (NZ * NP, ROWS), 0) == cl).astype(f32)
    upper[...] = (
        lax.broadcasted_iota(i32, (ROWS, ROWS), 0) < lax.broadcasted_iota(i32, (ROWS, ROWS), 1)
    ).astype(f32).astype(bf16)
    earlier = dot(one_hot.astype(bf16), upper[...], 1, 0)
    rank = jnp.sum(earlier * one_hot, axis=0, keepdims=True).astype(i32)
    slot_ref[...] = cl * DEPTH + rank
    lane = rank * NZ + cl // NP
    which[...] = (lax.broadcasted_iota(i32, (NP, ROWS), 0) == lax.rem(cl, NP)).astype(f32).astype(bf16)
    number = ix_ref[...] + 1
    mine = lax.broadcasted_iota(i32, (128, ROWS), 0) == lane
    total = jnp.zeros((NP, 128), f32)
    for part, weight in ((number // 4096, 4096.0), (lax.rem(number // 64, 64), 64.0), (lax.rem(number, 64), 1.0)):
        held = jnp.where(mine, part.astype(f32), 0.0).astype(bf16)
        total = total + weight * dot(which[...], held, 1, 1)
    idx_p[...] = total.reshape(NP, 1, 128)

    proj[...] = jnp.zeros((ROWS, PC), f32)

    @pl.loop(0, NEMB)
    def _(n):
        for copy in depth_in(n):
            copy.wait()
        part = pl.ds(pl.multiple_of(n * DEEP, DEEP), DEEP)
        proj[...] += jnp.dot(ebuf[:, part], bbuf[part, :], preferred_element_type=f32)

    for n in range(ROWS // EROWS):
        part = slice(n * EROWS, (n + 1) * EROWS)
        projected = proj[part, :]
        scale = lax.rsqrt(jnp.sum(projected * projected, axis=1, keepdims=True) + 1e-06)
        unit[part, :] = (projected * scale).astype(bf16)

    pl.semaphore_wait(barrier, NZ - 1 + NP - 1)

    def own_lanes():
        return lax.broadcasted_iota(i32, (BLK, 128), 1) // NZ == lax.rem(
            lax.broadcasted_iota(i32, (BLK, 128), 0), DEPTH
        )

    def pass_numbers():
        wait_bytes(all_but_one(idx_in), ip_r)
        wide = jnp.broadcast_to(idx_in[...], (NP, DEPTH, 128)).reshape(BLK, 128)
        keep = own_lanes()
        turned = jnp.where(keep, wide, 0.0).T.reshape(128 // NZ, NZ, BLK).sum(axis=0)
        for k in range(NZ):
            idx_z[k] = turned[k : k + 1, :]
        for k, step in enumerate(ORDER):
            if step:
                to_z(idx_z.at[turn_z(step)], idx_rec.at[k], iz_s, iz_r, turn_z(step))
            else:
                idx_rec[k] = idx_z[z]

    def onward(j):
        k = slot_of(j)
        z2 = turn_z(step_of(j))
        wait_bytes(all_but_one(recv1.at[z2]), rp_r.at[z2])
        to_z(recv1.at[z2], fin.at[k], rz_s.at[k], fin_r.at[k], z2)

    far = turn_z(ORDER[FAR])

    @pl.loop(0, NZ)
    def _(j):
        z2 = turn_z(step_of(j))
        picks = (lax.broadcasted_iota(i32, (BLK, ROWS), 0) == slot_ref[...] - z2 * BLK).astype(f32)
        chosen = jnp.dot(picks.astype(bf16), unit[...], preferred_element_type=f32)
        send[z2] = chosen.reshape(NP, DEPTH, PC).astype(bf16)

        @pl.when(j == 0)
        def _():
            to_z(send.at[far], zin, zi_s, zi_r, far)
            to_plane(idx_p, idx_in, ip_s, ip_r)

        @pl.when(j > 0)
        def _():
            to_plane(send.at[z2], recv1.at[z2], rp_s, rp_r.at[z2])

        @pl.when(j == 4)
        def _():
            pass_numbers()

        @pl.when(j >= 4)
        def _():
            onward(j - 3)

    wait_bytes(zin, zi_r)
    to_plane(zin, fin.at[FAR], fw_s, fin_r.at[FAR])

    @pl.loop(5, NZ - 1)
    def _(j):
        onward(j)

    wait_bytes(idx_rec.at[pl.ds(0, NZ - 1)], iz_r)

    @pl.loop(0, NZ)
    def _(k):
        row = idx_rec[k]
        row = jnp.where(row == 0.0, BIG, row)
        idx_rec[k] = row
        col[k] = jnp.broadcast_to(row, (128, BLK)).T
        colnow[k] = jnp.full((BLK, 128), BIG, f32)
        rows[k] = jnp.zeros((BLK, PC), bf16)
        bestcol[k] = jnp.full((BLK, 128), -1.0, f32)

    wait_bytes(all_but_one(recv1.at[z]), rp_r.at[z])
    fin[0] = recv1[z]

    @pl.loop(0, NZ)
    def _(k):
        @pl.when(k == FAR)
        def _():
            wait_bytes(all_but_one(fin.at[FAR]), fin_r.at[FAR])

        @pl.when(jnp.logical_and(k > 0, k != FAR))
        def _():
            wait_bytes(fin.at[k], fin_r.at[k])

        rows[k] = fin[k].reshape(BLK, PC)
        colnow[k] = col[k]
        ra = idx_rec[k]
        met = rows[k]
        over_rows = [None] * (BLK // 128)
        for b in range(NZ):
            scores = dot(rows[b], met, 1, 1)
            cb = colnow[b]
            over_cols = bestcol[b]
            for h in range(BLK // 128):
                lanes = slice(h * 128, (h + 1) * 128)
                s = scores[:, lanes]
                r = ra[:, lanes]
                earlier = cb < r
                own = jnp.max(jnp.where(earlier, s, -1.0).reshape(BLK // 8, 8, 128), axis=0)
                over_rows[h] = own if b == 0 else jnp.maximum(over_rows[h], own)
                over_cols = jnp.maximum(over_cols, jnp.where(earlier, -1.0, s))
            bestcol[b] = over_cols
        best[k] = jnp.concatenate(over_rows, axis=1)
        bestcol[k] = jnp.full((BLK, 128), -1.0, f32)

    finals = [
        jnp.maximum(
            jnp.max(best[k], axis=0, keepdims=True), jnp.max(bestcol[k].T, axis=0, keepdims=True)
        )
        for k in range(NZ)
    ]
    for k in range(1, NZ):
        ret_row[k] = finals[k]
    for k in range(1, NZ):
        to_z(ret_row.at[k], ret_z.at[z], bz_s, bz_r, turn_z(NZ - ORDER[k]))
    ret_z[z] = finals[0]
    wait_bytes(ret_z.at[pl.ds(0, NZ - 1)], bz_r)
    stacked = ret_z[...].reshape(NZ, BLK)
    spread = jnp.concatenate([stacked] * (128 // NZ), axis=0).T
    ret_p[...] = jnp.where(own_lanes(), spread, 0.0).reshape(NP, DEPTH, 128).sum(axis=1, keepdims=True)
    to_plane(ret_p, ret_c, bp_s, bp_r)
    wait_bytes(all_but_one(ret_c), bp_r)
    whole = ret_c[...].reshape(NP, 128).T[: NZ * DEPTH, :]
    high = whole.astype(bf16)
    rest = whole - high.astype(f32)
    mid = rest.astype(bf16)
    low = (rest - mid.astype(f32)).astype(bf16)
    got = jnp.zeros((NZ * DEPTH, ROWS), f32)
    for piece in (high, mid, low):
        got = got + jnp.dot(piece, which[...], preferred_element_type=f32)
    slots = slot_ref[...]
    lanes = lax.rem(slots, DEPTH) * NZ + slots // BLK
    mask = lax.broadcasted_iota(i32, (NZ * DEPTH, ROWS), 0) == lanes
    out_ref[...] = jnp.sum(jnp.where(mask, got, 0.0), axis=0, keepdims=True)

    wait_bytes(all_but_one(idx_p), ip_s)
    wait_bytes(idx_z.at[pl.ds(0, NZ - 1)], iz_s)
    wait_bytes(send.at[pl.ds(0, NZ - 1), pl.ds(0, NP - 1)], rp_s)
    wait_bytes(zin, zi_s)
    wait_bytes(all_but_one(zin), fw_s)
    for k in range(1, NZ):
        if k != FAR:
            wait_bytes(fin.at[k], rz_s.at[k])
    wait_bytes(ret_row.at[pl.ds(0, NZ - 1)], bz_s)
    wait_bytes(all_but_one(ret_p), bp_s)


def on_device(embeddings, pca_basis, cluster, doc_index):
    vmem = pl.BlockSpec(memory_space=pltpu.VMEM)
    hbm = pl.BlockSpec(memory_space=pl.ANY)
    dma = pltpu.SemaphoreType.DMA
    out = pl.pallas_call(
        kernel,
        out_shape=jax.ShapeDtypeStruct((1, ROWS), f32),
        in_specs=[hbm, hbm, hbm, hbm],
        out_specs=vmem,
        scratch_shapes=[
            pltpu.VMEM((1, ROWS), i32),
            pltpu.VMEM((1, ROWS), i32),
            pltpu.VMEM((ROWS, E), bf16),
            pltpu.VMEM((E, PC), bf16),
            pltpu.VMEM((ROWS, PC), f32),
            pltpu.VMEM((ROWS, PC), bf16),
            pltpu.VMEM((NP, ROWS), bf16),
            pltpu.VMEM((ROWS, ROWS), bf16),
            pltpu.VMEM((1, ROWS), i32),
            pltpu.VMEM((NP, 1, 128), f32),
            pltpu.VMEM((NP, 1, 128), f32),
            pltpu.VMEM((NZ, 1, BLK), f32),
            pltpu.VMEM((NZ, 1, BLK), f32),
            pltpu.VMEM((NZ, BLK, 128), f32),
            pltpu.VMEM((NZ, BLK, 128), f32),
            pltpu.VMEM((NZ, NP, DEPTH, PC), bf16),
            pltpu.VMEM((NZ, NP, DEPTH, PC), bf16),
            pltpu.VMEM((NP, DEPTH, PC), bf16),
            pltpu.VMEM((NZ, NP, DEPTH, PC), bf16),
            pltpu.VMEM((NZ, BLK, PC), bf16),
            pltpu.VMEM((NZ, 8, BLK), f32),
            pltpu.VMEM((NZ, BLK, 128), f32),
            pltpu.VMEM((NZ, 1, BLK), f32),
            pltpu.VMEM((NZ, 1, BLK), f32),
            pltpu.VMEM((NP, 1, 128), f32),
            pltpu.VMEM((NP, 1, 128), f32),
            dma((2,)), dma((NEMB,)), dma((NEMB,)), dma, dma, dma, dma, dma, dma((NZ,)), dma, dma,
            dma, dma((NZ,)), dma((NZ,)), dma, dma, dma, dma,
        ],
        compiler_params=pltpu.CompilerParams(
            collective_id=0, has_side_effects=True, vmem_limit_bytes=60 * 2**20
        ),
    )(cluster.reshape(1, ROWS), doc_index.reshape(1, ROWS), embeddings, pca_basis)
    return out.reshape(ROWS)


def solution(mesh):
    return jax.shard_map(
        on_device,
        mesh=mesh,
        in_specs=(P(("docs", "rep"), None), P(), P(("docs", "rep"), None), P(("docs", "rep"))),
        out_specs=P(("docs", "rep")),
        check_vma=False,
    )
```

```python
import jax
import jax.numpy as jnp
from jax import lax
from jax.experimental import pallas as pl
from jax.experimental.pallas import tpu as pltpu
from jax.sharding import PartitionSpec as P

MESH = pl.DeviceIdType.MESH
NX, NY, NZ, NC = 4, 4, 8, 2
NP = NX * NY * NC
DEPTH = 8
ROWS = 1024
PC = 256
E = 4096
BLK = NP * DEPTH
NEMB = 8
EARLY = 0
DEEP = E // NEMB
EROWS = 256
ORDER = (0, 4, 2, 6, 3, 5, 1, 7)
FAR = (1, 4, 5)
NFAR = 3
BIG = float(2**30)
f32, bf16, i32 = jnp.float32, jnp.bfloat16, jnp.int32


def dot(a, b, ca, cb):
    return lax.dot_general(a, b, (((ca,), (cb,)), ((), ())), preferred_element_type=f32)


def step_of(j):
    return NZ // 2 + (1 - 2 * (j % 2)) * ((j + 1) // 2)


def slot_of(j):
    return j - 1 + 2 * (j // 5)


def wait_bytes(ref, sem):
    pltpu.make_async_copy(ref, ref, sem).wait()


def kernel(
    cl_hbm, ix_hbm, emb_ref, bas_ref, out_ref,
    cl_ref, ix_ref, ebuf, bbuf, proj, unit, which, upper, slot_ref,
    idx_p, idx_in, idx_z, idx_rec, col, colnow,
    send, recv1, zin, fin, rows, best, bestcol,
    ret_row, ret_z, ret_p, ret_c,
    n_sem, e_sem, b_sem, ip_s, ip_r, iz_s, iz_r, rp_s, rp_r, zi_s, zi_r, fw_s, fin_r, rz_s,
    bz_s, bz_r, bp_s, bp_r,
):
    d = lax.axis_index("docs")
    y = lax.axis_index("rep")
    core = lax.rem(d, NC)
    z = lax.rem(d // NC, NZ)
    x = d // (NC * NZ)
    p = (x * NY + y) * NC + core

    def at_z(z2):
        return ((x * NZ + z2) * NC + core, y)

    def turn_z(step):
        return lax.rem(z + step, NZ)

    beside = [
        (lax.rem(y + ky, NY), lax.rem(core + kc, NC)) for ky in range(NY) for kc in range(NC)
    ]
    beside = [(y2, y2 * NC + c2, z * NC + c2) for y2, c2 in beside]

    def each_beside(fn):
        def of_column(x2, some):
            for y2, place, deep in some:
                fn(x2 * (NY * NC) + place, (x2 * (NZ * NC) + deep, y2))

        of_column(x, beside[1:])

        @pl.loop(1, NX)
        def _(kx):
            of_column(lax.rem(x + kx, NX), beside)

    def to_z(src, dst, send_sem, recv_sem, z2):
        pltpu.make_async_remote_copy(
            src_ref=src, dst_ref=dst, send_sem=send_sem, recv_sem=recv_sem,
            device_id=at_z(z2), device_id_type=MESH,
        ).start()

    def to_plane(src, dst, send_sem, recv_sem):
        def to_one(p2, device):
            pltpu.make_async_remote_copy(
                src_ref=src.at[p2], dst_ref=dst.at[p], send_sem=send_sem, recv_sem=recv_sem,
                device_id=device, device_id_type=MESH,
            ).start()

        each_beside(to_one)
        dst[p] = src[p]

    def all_but_one(ref):
        return ref.at[pl.ds(0, NP - 1)]

    cl_copy = pltpu.make_async_copy(cl_hbm, cl_ref, n_sem.at[0])
    ix_copy = pltpu.make_async_copy(ix_hbm, ix_ref, n_sem.at[1])
    cl_copy.start()
    ix_copy.start()
    def depth_in(n):
        part = pl.ds(pl.multiple_of(n * DEEP, DEEP), DEEP)
        return (
            pltpu.make_async_copy(bas_ref.at[part], bbuf.at[part], b_sem.at[n]),
            pltpu.make_async_copy(emb_ref.at[:, part], ebuf.at[:, part], e_sem.at[n]),
        )

    for n in range(EARLY):
        for copy in depth_in(n):
            copy.start()
    barrier = pltpu.get_barrier_semaphore()
    for step in range(1, NZ):
        pl.semaphore_signal(barrier, inc=1, device_id=at_z(turn_z(step)), device_id_type=MESH)

    each_beside(
        lambda p2, device: pl.semaphore_signal(barrier, inc=1, device_id=device, device_id_type=MESH)
    )

    cl_copy.wait()
    ix_copy.wait()
    for n in range(EARLY, NEMB):
        for copy in depth_in(n):
            copy.start()
    cl = cl_ref[...]
    one_hot = (lax.broadcasted_iota(i32, (NZ * NP, ROWS), 0) == cl).astype(f32)
    upper[...] = (
        lax.broadcasted_iota(i32, (ROWS, ROWS), 0) < lax.broadcasted_iota(i32, (ROWS, ROWS), 1)
    ).astype(f32).astype(bf16)
    earlier = dot(one_hot.astype(bf16), upper[...], 1, 0)
    rank = jnp.sum(earlier * one_hot, axis=0, keepdims=True).astype(i32)
    slot_ref[...] = cl * DEPTH + rank
    lane = rank * NZ + cl // NP
    which[...] = (lax.broadcasted_iota(i32, (NP, ROWS), 0) == lax.rem(cl, NP)).astype(f32).astype(bf16)
    number = ix_ref[...] + 1
    mine = lax.broadcasted_iota(i32, (128, ROWS), 0) == lane
    total = jnp.zeros((NP, 128), f32)
    for part, weight in ((number // 4096, 4096.0), (lax.rem(number // 64, 64), 64.0), (lax.rem(number, 64), 1.0)):
        held = jnp.where(mine, part.astype(f32), 0.0).astype(bf16)
        total = total + weight * dot(which[...], held, 1, 1)
    idx_p[...] = total.reshape(NP, 1, 128)

    proj[...] = jnp.zeros((ROWS, PC), f32)

    @pl.loop(0, NEMB)
    def _(n):
        for copy in depth_in(n):
            copy.wait()
        part = pl.ds(pl.multiple_of(n * DEEP, DEEP), DEEP)
        proj[...] += jnp.dot(ebuf[:, part], bbuf[part, :], preferred_element_type=f32)

    for n in range(ROWS // EROWS):
        part = slice(n * EROWS, (n + 1) * EROWS)
        projected = proj[part, :]
        scale = lax.rsqrt(jnp.sum(projected * projected, axis=1, keepdims=True) + 1e-06)
        unit[part, :] = (projected * scale).astype(bf16)

    pl.semaphore_wait(barrier, NZ - 1 + NP - 1)

    def own_lanes():
        return lax.broadcasted_iota(i32, (BLK, 128), 1) // NZ == lax.rem(
            lax.broadcasted_iota(i32, (BLK, 128), 0), DEPTH
        )

    def pass_numbers():
        wait_bytes(all_but_one(idx_in), ip_r)
        wide = jnp.broadcast_to(idx_in[...], (NP, DEPTH, 128)).reshape(BLK, 128)
        keep = own_lanes()
        turned = jnp.where(keep, wide, 0.0).T.reshape(128 // NZ, NZ, BLK).sum(axis=0)
        for k in range(NZ):
            idx_z[k] = turned[k : k + 1, :]
        for k, step in enumerate(ORDER):
            if step:
                to_z(idx_z.at[turn_z(step)], idx_rec.at[k], iz_s, iz_r, turn_z(step))
            else:
                idx_rec[k] = idx_z[z]

    def onward(j):
        k = slot_of(j)
        z2 = turn_z(step_of(j))
        wait_bytes(all_but_one(recv1.at[z2]), rp_r.at[z2])
        to_z(recv1.at[z2], fin.at[k], rz_s.at[k], fin_r.at[k], z2)

    @pl.loop(0, NZ)
    def _(j):
        z2 = turn_z(step_of(j))
        picks = (lax.broadcasted_iota(i32, (BLK, ROWS), 0) == slot_ref[...] - z2 * BLK).astype(f32)
        chosen = jnp.dot(picks.astype(bf16), unit[...], preferred_element_type=f32)
        send[z2] = chosen.reshape(NP, DEPTH, PC).astype(bf16)

        @pl.when(j < NFAR)
        def _():
            to_z(send.at[z2], zin.at[j], zi_s.at[j], zi_r.at[j], z2)

        @pl.when(j == 0)
        def _():
            to_plane(idx_p, idx_in, ip_s, ip_r)

        @pl.when(j >= NFAR)
        def _():
            to_plane(send.at[z2], recv1.at[z2], rp_s, rp_r.at[z2])

        @pl.when(j == 6)
        def _():
            pass_numbers()


    @pl.loop(NFAR, NZ - 1)
    def _(j):
        onward(j)

    for j, k in enumerate(FAR):
        wait_bytes(zin.at[j], zi_r.at[j])
        to_plane(zin.at[j], fin.at[k], fw_s, fin_r.at[k])

    wait_bytes(idx_rec.at[pl.ds(0, NZ - 1)], iz_r)

    @pl.loop(0, NZ)
    def _(k):
        row = idx_rec[k]
        row = jnp.where(row == 0.0, BIG, row)
        idx_rec[k] = row
        col[k] = jnp.broadcast_to(row, (128, BLK)).T
        colnow[k] = jnp.full((BLK, 128), BIG, f32)
        rows[k] = jnp.zeros((BLK, PC), bf16)
        bestcol[k] = jnp.full((BLK, 128), -1.0, f32)

    wait_bytes(all_but_one(recv1.at[z]), rp_r.at[z])
    fin[0] = recv1[z]

    @pl.loop(0, NZ)
    def _(k):
        far = jnp.logical_or(k == FAR[0], jnp.logical_and(k >= FAR[1], k <= FAR[2]))

        @pl.when(far)
        def _():
            wait_bytes(all_but_one(fin.at[k]), fin_r.at[k])

        @pl.when(jnp.logical_and(k > 0, jnp.logical_not(far)))
        def _():
            wait_bytes(fin.at[k], fin_r.at[k])

        rows[k] = fin[k].reshape(BLK, PC)
        colnow[k] = col[k]
        ra = idx_rec[k]
        met = rows[k]
        over_rows = [None] * (BLK // 128)
        for b in range(NZ):
            scores = dot(rows[b], met, 1, 1)
            cb = colnow[b]
            over_cols = bestcol[b]
            for h in range(BLK // 128):
                lanes = slice(h * 128, (h + 1) * 128)
                s = scores[:, lanes]
                r = ra[:, lanes]
                earlier = cb < r
                own = jnp.max(jnp.where(earlier, s, -1.0).reshape(BLK // 8, 8, 128), axis=0)
                over_rows[h] = own if b == 0 else jnp.maximum(over_rows[h], own)
                over_cols = jnp.maximum(over_cols, jnp.where(earlier, -1.0, s))
            bestcol[b] = over_cols
        best[k] = jnp.concatenate(over_rows, axis=1)
        bestcol[k] = jnp.full((BLK, 128), -1.0, f32)

    finals = [
        jnp.maximum(
            jnp.max(best[k], axis=0, keepdims=True), jnp.max(bestcol[k].T, axis=0, keepdims=True)
        )
        for k in range(NZ)
    ]
    for k in range(1, NZ):
        ret_row[k] = finals[k]
    for k in range(1, NZ):
        to_z(ret_row.at[k], ret_z.at[z], bz_s, bz_r, turn_z(NZ - ORDER[k]))
    ret_z[z] = finals[0]
    wait_bytes(ret_z.at[pl.ds(0, NZ - 1)], bz_r)
    stacked = ret_z[...].reshape(NZ, BLK)
    spread = jnp.concatenate([stacked] * (128 // NZ), axis=0).T
    ret_p[...] = jnp.where(own_lanes(), spread, 0.0).reshape(NP, DEPTH, 128).sum(axis=1, keepdims=True)
    to_plane(ret_p, ret_c, bp_s, bp_r)
    wait_bytes(all_but_one(ret_c), bp_r)
    whole = ret_c[...].reshape(NP, 128).T[: NZ * DEPTH, :]
    high = whole.astype(bf16)
    rest = whole - high.astype(f32)
    mid = rest.astype(bf16)
    low = (rest - mid.astype(f32)).astype(bf16)
    got = jnp.zeros((NZ * DEPTH, ROWS), f32)
    for piece in (high, mid, low):
        got = got + jnp.dot(piece, which[...], preferred_element_type=f32)
    slots = slot_ref[...]
    lanes = lax.rem(slots, DEPTH) * NZ + slots // BLK
    mask = lax.broadcasted_iota(i32, (NZ * DEPTH, ROWS), 0) == lanes
    out_ref[...] = jnp.sum(jnp.where(mask, got, 0.0), axis=0, keepdims=True)

    wait_bytes(all_but_one(idx_p), ip_s)
    wait_bytes(idx_z.at[pl.ds(0, NZ - 1)], iz_s)
    wait_bytes(send.at[pl.ds(0, NZ - NFAR), pl.ds(0, NP - 1)], rp_s)
    for j in range(NFAR):
        wait_bytes(zin.at[j], zi_s.at[j])
    wait_bytes(zin.at[:, pl.ds(0, NP - 1)], fw_s)
    for k in range(1, NZ):
        if k not in FAR:
            wait_bytes(fin.at[k], rz_s.at[k])
    wait_bytes(ret_row.at[pl.ds(0, NZ - 1)], bz_s)
    wait_bytes(all_but_one(ret_p), bp_s)


def on_device(embeddings, pca_basis, cluster, doc_index):
    vmem = pl.BlockSpec(memory_space=pltpu.VMEM)
    hbm = pl.BlockSpec(memory_space=pl.ANY)
    dma = pltpu.SemaphoreType.DMA
    out = pl.pallas_call(
        kernel,
        out_shape=jax.ShapeDtypeStruct((1, ROWS), f32),
        in_specs=[hbm, hbm, hbm, hbm],
        out_specs=vmem,
        scratch_shapes=[
            pltpu.VMEM((1, ROWS), i32),
            pltpu.VMEM((1, ROWS), i32),
            pltpu.VMEM((ROWS, E), bf16),
            pltpu.VMEM((E, PC), bf16),
            pltpu.VMEM((ROWS, PC), f32),
            pltpu.VMEM((ROWS, PC), bf16),
            pltpu.VMEM((NP, ROWS), bf16),
            pltpu.VMEM((ROWS, ROWS), bf16),
            pltpu.VMEM((1, ROWS), i32),
            pltpu.VMEM((NP, 1, 128), f32),
            pltpu.VMEM((NP, 1, 128), f32),
            pltpu.VMEM((NZ, 1, BLK), f32),
            pltpu.VMEM((NZ, 1, BLK), f32),
            pltpu.VMEM((NZ, BLK, 128), f32),
            pltpu.VMEM((NZ, BLK, 128), f32),
            pltpu.VMEM((NZ, NP, DEPTH, PC), bf16),
            pltpu.VMEM((NZ, NP, DEPTH, PC), bf16),
            pltpu.VMEM((NFAR, NP, DEPTH, PC), bf16),
            pltpu.VMEM((NZ, NP, DEPTH, PC), bf16),
            pltpu.VMEM((NZ, BLK, PC), bf16),
            pltpu.VMEM((NZ, 8, BLK), f32),
            pltpu.VMEM((NZ, BLK, 128), f32),
            pltpu.VMEM((NZ, 1, BLK), f32),
            pltpu.VMEM((NZ, 1, BLK), f32),
            pltpu.VMEM((NP, 1, 128), f32),
            pltpu.VMEM((NP, 1, 128), f32),
            dma((2,)), dma((NEMB,)), dma((NEMB,)), dma, dma, dma, dma, dma, dma((NZ,)), dma((NFAR,)), dma((NFAR,)),
            dma, dma((NZ,)), dma((NZ,)), dma, dma, dma, dma,
        ],
        compiler_params=pltpu.CompilerParams(
            collective_id=0, has_side_effects=True, vmem_limit_bytes=60 * 2**20
        ),
    )(cluster.reshape(1, ROWS), doc_index.reshape(1, ROWS), embeddings, pca_basis)
    return out.reshape(ROWS)


def solution(mesh):
    return jax.shard_map(
        on_device,
        mesh=mesh,
        in_specs=(P(("docs", "rep"), None), P(), P(("docs", "rep"), None), P(("docs", "rep"))),
        out_specs=P(("docs", "rep")),
        check_vma=False,
    )
```

```python
import jax
import jax.numpy as jnp
from jax import lax
from jax.experimental import pallas as pl
from jax.experimental.pallas import tpu as pltpu
from jax.sharding import PartitionSpec as P

MESH = pl.DeviceIdType.MESH
NX, NY, NZ, NC = 4, 4, 8, 2
NP = NX * NY * NC
DEPTH = 8
ROWS = 1024
PC = 256
E = 4096
BLK = NP * DEPTH
NEMB = 4
EARLY = 1
DEEP = E // NEMB
EROWS = 256
ORDER = (0, 4, 2, 6, 3, 5, 1, 7)
FAR = (1, 4, 5)
NFAR = 3
BIG = float(2**30)
f32, bf16, i32 = jnp.float32, jnp.bfloat16, jnp.int32


def dot(a, b, ca, cb):
    return lax.dot_general(a, b, (((ca,), (cb,)), ((), ())), preferred_element_type=f32)


def step_of(j):
    return NZ // 2 + (1 - 2 * (j % 2)) * ((j + 1) // 2)


def slot_of(j):
    return j - 1 + 2 * (j // 5)


def wait_bytes(ref, sem):
    pltpu.make_async_copy(ref, ref, sem).wait()


def kernel(
    cl_hbm, ix_hbm, emb_ref, bas_ref, out_ref,
    cl_ref, ix_ref, ebuf, bbuf, proj, unit, which, upper, slot_ref,
    idx_p, idx_in, idx_z, idx_rec, col, colnow,
    send, recv1, zin, fin, rows, best, bestcol,
    ret_row, ret_z, ret_p, ret_c,
    n_sem, e_sem, b_sem, ip_s, ip_r, iz_s, iz_r, rp_s, rp_r, zi_s, zi_r, fw_s, fin_r, rz_s,
    bz_s, bz_r, bp_s, bp_r,
):
    d = lax.axis_index("docs")
    y = lax.axis_index("rep")
    core = lax.rem(d, NC)
    z = lax.rem(d // NC, NZ)
    x = d // (NC * NZ)
    p = (x * NY + y) * NC + core

    def at_z(z2):
        return ((x * NZ + z2) * NC + core, y)

    def turn_z(step):
        return lax.rem(z + step, NZ)

    beside = [
        (lax.rem(y + ky, NY), lax.rem(core + kc, NC)) for ky in range(NY) for kc in range(NC)
    ]
    beside = [(y2, y2 * NC + c2, z * NC + c2) for y2, c2 in beside]

    def each_beside(fn):
        def of_column(x2, some):
            for y2, place, deep in some:
                fn(x2 * (NY * NC) + place, (x2 * (NZ * NC) + deep, y2))

        of_column(x, beside[1:])

        @pl.loop(1, NX)
        def _(kx):
            of_column(lax.rem(x + kx, NX), beside)

    def to_z(src, dst, send_sem, recv_sem, z2):
        pltpu.make_async_remote_copy(
            src_ref=src, dst_ref=dst, send_sem=send_sem, recv_sem=recv_sem,
            device_id=at_z(z2), device_id_type=MESH,
        ).start()

    def to_plane(src, dst, send_sem, recv_sem):
        def to_one(p2, device):
            pltpu.make_async_remote_copy(
                src_ref=src.at[p2], dst_ref=dst.at[p], send_sem=send_sem, recv_sem=recv_sem,
                device_id=device, device_id_type=MESH,
            ).start()

        each_beside(to_one)
        dst[p] = src[p]

    def all_but_one(ref):
        return ref.at[pl.ds(0, NP - 1)]

    cl_copy = pltpu.make_async_copy(cl_hbm, cl_ref, n_sem.at[0])
    ix_copy = pltpu.make_async_copy(ix_hbm, ix_ref, n_sem.at[1])
    cl_copy.start()
    ix_copy.start()
    def depth_in(n):
        part = pl.ds(pl.multiple_of(n * DEEP, DEEP), DEEP)
        return (
            pltpu.make_async_copy(bas_ref.at[part], bbuf.at[part], b_sem.at[n]),
            pltpu.make_async_copy(emb_ref.at[:, part], ebuf.at[:, part], e_sem.at[n]),
        )

    for n in range(EARLY):
        for copy in depth_in(n):
            copy.start()
    barrier = pltpu.get_barrier_semaphore()
    for step in range(1, NZ):
        pl.semaphore_signal(barrier, inc=1, device_id=at_z(turn_z(step)), device_id_type=MESH)

    each_beside(
        lambda p2, device: pl.semaphore_signal(barrier, inc=1, device_id=device, device_id_type=MESH)
    )

    cl_copy.wait()
    ix_copy.wait()
    for n in range(EARLY, NEMB):
        for copy in depth_in(n):
            copy.start()
    cl = cl_ref[...]
    one_hot = (lax.broadcasted_iota(i32, (NZ * NP, ROWS), 0) == cl).astype(f32)
    upper[...] = (
        lax.broadcasted_iota(i32, (ROWS, ROWS), 0) < lax.broadcasted_iota(i32, (ROWS, ROWS), 1)
    ).astype(f32).astype(bf16)
    earlier = dot(one_hot.astype(bf16), upper[...], 1, 0)
    rank = jnp.sum(earlier * one_hot, axis=0, keepdims=True).astype(i32)
    slot_ref[...] = cl * DEPTH + rank
    lane = rank * NZ + cl // NP
    which[...] = (lax.broadcasted_iota(i32, (NP, ROWS), 0) == lax.rem(cl, NP)).astype(f32).astype(bf16)
    number = ix_ref[...] + 1
    mine = lax.broadcasted_iota(i32, (128, ROWS), 0) == lane
    total = jnp.zeros((NP, 128), f32)
    for part, weight in ((number // 4096, 4096.0), (lax.rem(number // 64, 64), 64.0), (lax.rem(number, 64), 1.0)):
        held = jnp.where(mine, part.astype(f32), 0.0).astype(bf16)
        total = total + weight * dot(which[...], held, 1, 1)
    idx_p[...] = total.reshape(NP, 1, 128)

    proj[...] = jnp.zeros((ROWS, PC), f32)

    @pl.loop(0, NEMB)
    def _(n):
        for copy in depth_in(n):
            copy.wait()
        part = pl.ds(pl.multiple_of(n * DEEP, DEEP), DEEP)
        proj[...] += jnp.dot(ebuf[:, part], bbuf[part, :], preferred_element_type=f32)

    for n in range(ROWS // EROWS):
        part = slice(n * EROWS, (n + 1) * EROWS)
        projected = proj[part, :]
        scale = lax.rsqrt(jnp.sum(projected * projected, axis=1, keepdims=True) + 1e-06)
        unit[part, :] = (projected * scale).astype(bf16)

    pl.semaphore_wait(barrier, NZ - 1 + NP - 1)

    def own_lanes():
        return lax.broadcasted_iota(i32, (BLK, 128), 1) // NZ == lax.rem(
            lax.broadcasted_iota(i32, (BLK, 128), 0), DEPTH
        )

    def pass_numbers():
        wait_bytes(all_but_one(idx_in), ip_r)
        wide = jnp.broadcast_to(idx_in[...], (NP, DEPTH, 128)).reshape(BLK, 128)
        keep = own_lanes()
        turned = jnp.where(keep, wide, 0.0).T.reshape(128 // NZ, NZ, BLK).sum(axis=0)
        for k in range(NZ):
            idx_z[k] = turned[k : k + 1, :]
        for k, step in enumerate(ORDER):
            if step:
                to_z(idx_z.at[turn_z(step)], idx_rec.at[k], iz_s, iz_r, turn_z(step))
            else:
                idx_rec[k] = idx_z[z]

    def onward(j):
        k = slot_of(j)
        z2 = turn_z(step_of(j))
        wait_bytes(all_but_one(recv1.at[z2]), rp_r.at[z2])
        to_z(recv1.at[z2], fin.at[k], rz_s.at[k], fin_r.at[k], z2)

    @pl.loop(0, NZ)
    def _(j):
        z2 = turn_z(step_of(j))
        picks = (lax.broadcasted_iota(i32, (BLK, ROWS), 0) == slot_ref[...] - z2 * BLK).astype(f32)
        chosen = jnp.dot(picks.astype(bf16), unit[...], preferred_element_type=f32)
        send[z2] = chosen.reshape(NP, DEPTH, PC).astype(bf16)

        @pl.when(j < NFAR)
        def _():
            to_z(send.at[z2], zin.at[j], zi_s.at[j], zi_r.at[j], z2)

        @pl.when(j == 0)
        def _():
            to_plane(idx_p, idx_in, ip_s, ip_r)

        @pl.when(j >= NFAR)
        def _():
            to_plane(send.at[z2], recv1.at[z2], rp_s, rp_r.at[z2])

        @pl.when(j == 6)
        def _():
            pass_numbers()


    @pl.loop(NFAR, NZ - 1)
    def _(j):
        onward(j)

    for j, k in enumerate(FAR):
        wait_bytes(zin.at[j], zi_r.at[j])
        to_plane(zin.at[j], fin.at[k], fw_s, fin_r.at[k])

    wait_bytes(idx_rec.at[pl.ds(0, NZ - 1)], iz_r)

    @pl.loop(0, NZ)
    def _(k):
        row = idx_rec[k]
        row = jnp.where(row == 0.0, BIG, row)
        idx_rec[k] = row
        col[k] = jnp.broadcast_to(row, (128, BLK)).T
        colnow[k] = jnp.full((BLK, 128), BIG, f32)
        rows[k] = jnp.zeros((BLK, PC), bf16)
        bestcol[k] = jnp.full((BLK, 128), -1.0, f32)

    wait_bytes(all_but_one(recv1.at[z]), rp_r.at[z])
    fin[0] = recv1[z]

    @pl.loop(0, NZ)
    def _(k):
        far = jnp.logical_or(k == FAR[0], jnp.logical_and(k >= FAR[1], k <= FAR[2]))

        @pl.when(far)
        def _():
            wait_bytes(all_but_one(fin.at[k]), fin_r.at[k])

        @pl.when(jnp.logical_and(k > 0, jnp.logical_not(far)))
        def _():
            wait_bytes(fin.at[k], fin_r.at[k])

        rows[k] = fin[k].reshape(BLK, PC)
        colnow[k] = col[k]
        ra = idx_rec[k]
        met = rows[k]
        over_rows = [None] * (BLK // 128)
        for b in range(NZ):
            scores = dot(rows[b], met, 1, 1)
            cb = colnow[b]
            over_cols = bestcol[b]
            for h in range(BLK // 128):
                lanes = slice(h * 128, (h + 1) * 128)
                s = scores[:, lanes]
                r = ra[:, lanes]
                earlier = cb < r
                own = jnp.max(jnp.where(earlier, s, -1.0).reshape(BLK // 8, 8, 128), axis=0)
                over_rows[h] = own if b == 0 else jnp.maximum(over_rows[h], own)
                over_cols = jnp.maximum(over_cols, jnp.where(earlier, -1.0, s))
            bestcol[b] = over_cols
        best[k] = jnp.concatenate(over_rows, axis=1)
        bestcol[k] = jnp.full((BLK, 128), -1.0, f32)

    finals = [
        jnp.maximum(
            jnp.max(best[k], axis=0, keepdims=True), jnp.max(bestcol[k].T, axis=0, keepdims=True)
        )
        for k in range(NZ)
    ]
    for k in range(1, NZ):
        ret_row[k] = finals[k]
    for k in range(1, NZ):
        to_z(ret_row.at[k], ret_z.at[z], bz_s, bz_r, turn_z(NZ - ORDER[k]))
    ret_z[z] = finals[0]
    wait_bytes(ret_z.at[pl.ds(0, NZ - 1)], bz_r)
    stacked = ret_z[...].reshape(NZ, BLK)
    spread = jnp.concatenate([stacked] * (128 // NZ), axis=0).T
    ret_p[...] = jnp.where(own_lanes(), spread, 0.0).reshape(NP, DEPTH, 128).sum(axis=1, keepdims=True)
    to_plane(ret_p, ret_c, bp_s, bp_r)
    wait_bytes(all_but_one(ret_c), bp_r)
    whole = ret_c[...].reshape(NP, 128).T[: NZ * DEPTH, :]
    high = whole.astype(bf16)
    rest = whole - high.astype(f32)
    mid = rest.astype(bf16)
    low = (rest - mid.astype(f32)).astype(bf16)
    got = jnp.zeros((NZ * DEPTH, ROWS), f32)
    for piece in (high, mid, low):
        got = got + jnp.dot(piece, which[...], preferred_element_type=f32)
    slots = slot_ref[...]
    lanes = lax.rem(slots, DEPTH) * NZ + slots // BLK
    mask = lax.broadcasted_iota(i32, (NZ * DEPTH, ROWS), 0) == lanes
    out_ref[...] = jnp.sum(jnp.where(mask, got, 0.0), axis=0, keepdims=True)

    wait_bytes(all_but_one(idx_p), ip_s)
    wait_bytes(idx_z.at[pl.ds(0, NZ - 1)], iz_s)
    wait_bytes(send.at[pl.ds(0, NZ - NFAR), pl.ds(0, NP - 1)], rp_s)
    for j in range(NFAR):
        wait_bytes(zin.at[j], zi_s.at[j])
    wait_bytes(zin.at[:, pl.ds(0, NP - 1)], fw_s)
    for k in range(1, NZ):
        if k not in FAR:
            wait_bytes(fin.at[k], rz_s.at[k])
    wait_bytes(ret_row.at[pl.ds(0, NZ - 1)], bz_s)
    wait_bytes(all_but_one(ret_p), bp_s)


def on_device(embeddings, pca_basis, cluster, doc_index):
    vmem = pl.BlockSpec(memory_space=pltpu.VMEM)
    hbm = pl.BlockSpec(memory_space=pl.ANY)
    dma = pltpu.SemaphoreType.DMA
    out = pl.pallas_call(
        kernel,
        out_shape=jax.ShapeDtypeStruct((1, ROWS), f32),
        in_specs=[hbm, hbm, hbm, hbm],
        out_specs=vmem,
        scratch_shapes=[
            pltpu.VMEM((1, ROWS), i32),
            pltpu.VMEM((1, ROWS), i32),
            pltpu.VMEM((ROWS, E), bf16),
            pltpu.VMEM((E, PC), bf16),
            pltpu.VMEM((ROWS, PC), f32),
            pltpu.VMEM((ROWS, PC), bf16),
            pltpu.VMEM((NP, ROWS), bf16),
            pltpu.VMEM((ROWS, ROWS), bf16),
            pltpu.VMEM((1, ROWS), i32),
            pltpu.VMEM((NP, 1, 128), f32),
            pltpu.VMEM((NP, 1, 128), f32),
            pltpu.VMEM((NZ, 1, BLK), f32),
            pltpu.VMEM((NZ, 1, BLK), f32),
            pltpu.VMEM((NZ, BLK, 128), f32),
            pltpu.VMEM((NZ, BLK, 128), f32),
            pltpu.VMEM((NZ, NP, DEPTH, PC), bf16),
            pltpu.VMEM((NZ, NP, DEPTH, PC), bf16),
            pltpu.VMEM((NFAR, NP, DEPTH, PC), bf16),
            pltpu.VMEM((NZ, NP, DEPTH, PC), bf16),
            pltpu.VMEM((NZ, BLK, PC), bf16),
            pltpu.VMEM((NZ, 8, BLK), f32),
            pltpu.VMEM((NZ, BLK, 128), f32),
            pltpu.VMEM((NZ, 1, BLK), f32),
            pltpu.VMEM((NZ, 1, BLK), f32),
            pltpu.VMEM((NP, 1, 128), f32),
            pltpu.VMEM((NP, 1, 128), f32),
            dma((2,)), dma((NEMB,)), dma((NEMB,)), dma, dma, dma, dma, dma, dma((NZ,)), dma((NFAR,)), dma((NFAR,)),
            dma, dma((NZ,)), dma((NZ,)), dma, dma, dma, dma,
        ],
        compiler_params=pltpu.CompilerParams(
            collective_id=0, has_side_effects=True, vmem_limit_bytes=60 * 2**20
        ),
    )(cluster.reshape(1, ROWS), doc_index.reshape(1, ROWS), embeddings, pca_basis)
    return out.reshape(ROWS)


def solution(mesh):
    return jax.shard_map(
        on_device,
        mesh=mesh,
        in_specs=(P(("docs", "rep"), None), P(), P(("docs", "rep"), None), P(("docs", "rep"))),
        out_specs=P(("docs", "rep")),
        check_vma=False,
    )
```
